32 devices in a mesh: job: 4 (over y, x), zero: 2 (over core), cols: 4 (over z).
Axes of the slice: x: 2, y: 2, z: 4, core: 2. Of those that a mesh axis runs over, the one named last changes fastest.
Arguments:
- weight_query: bfloat16 [12288, 3072], P(('job', 'zero'), 'cols'), parts along dimension 0, may hold values from -0.109375 to 0.109375
- low_query: bfloat16 [12288, 32], P(('job', 'zero')), parts along dimension 0, may hold values from -0.109375 to 0.109375
- high_query: bfloat16 [128, 3072], P('job', 'cols'), parts along dimension 0, may hold values from -1 to 1
- weight_key: bfloat16 [12288, 1024], P(('job', 'zero'), 'cols'), parts along dimension 0, may hold values from -0.109375 to 0.109375
- low_key: bfloat16 [12288, 32], P(('job', 'zero')), parts along dimension 0, may hold values from -0.109375 to 0.109375
- high_key: bfloat16 [128, 1024], P('job', 'cols'), parts along dimension 0, may hold values from -1 to 1
- weight_value: bfloat16 [12288, 1024], P(('job', 'zero'), 'cols'), parts along dimension 0, may hold values from -0.109375 to 0.109375
- low_value: bfloat16 [12288, 32], P(('job', 'zero')), parts along dimension 0, may hold values from -0.109375 to 0.109375
- high_value: bfloat16 [128, 1024], P('job', 'cols'), parts along dimension 0, may hold values from -1 to 1
- weight_mixed: bfloat16 [12288, 3072], P(('job', 'cols'), 'zero'), parts along dimension 0, may hold values from -0.109375 to 0.109375
- low_mixed: bfloat16 [12288, 32], P(('job', 'cols')), parts along dimension 0, may hold values from -0.109375 to 0.109375
- high_mixed: bfloat16 [128, 3072], P('job', 'zero'), parts along dimension 0, may hold values from -1 to 1
- norm_train: float32 [12288], P(('job', 'zero', 'cols')), parts along dimension 0, may hold values from 0.25 to 1.75
- norm_step: float32 [12288], P(('job', 'zero', 'cols')), parts along dimension 0, may hold values from -0.3 to 0.3
Outputs:
- serving_query: bfloat16 [12288, 3072], P('job', 'cols'), parts along dimension 0
- serving_key: bfloat16 [12288, 1024], P('job', 'cols'), parts along dimension 0
- serving_value: bfloat16 [12288, 1024], P('job', 'cols'), parts along dimension 0
- serving_mixed: bfloat16 [12288, 3072], P(('job', 'cols')), parts along dimension 0
- serve_norm: bfloat16 [12288], P('job'), parts along dimension 0
The draws below stay inside these ranges and needn't reach their ends.
There are 4 independent parts, one for each index of `job`. The reference program is written for one: setup_inputs(seed, part) draws one part's arguments, and reference() takes and returns one part's arrays. A program takes and returns all parts, laid end to end along the dimension named above; each array names one. Nothing has to cross between parts.
All inputs are finite; a program needn't handle non-finite values.
Results may differ from the reference program's by a relative error of at most 0.001.
Values may be sent and summed in bfloat16 or wider, within the bound.
No kernel may reach another device: no remote copies, remote signals or barrier semaphores. Data moves between devices by JAX's collectives and lax.ppermute only.
A program may use at most 128 MiB of HBM per device.

```python
import jax
import jax.numpy as jnp

D_MODEL = 3072
Q_DIM = 3072
KV_DIM = 1024
RANK = 32


def shard_levels(own_key, extent, split, smallest, high):
    def one(axis_at, shards_of):
        draws = jax.random.uniform(jax.random.fold_in(jax.random.fold_in(own_key, 6), axis_at), (shards_of,), jnp.float32, smallest / len(split), high / len(split))
        return jnp.repeat(jnp.exp(draws), extent[axis_at] // shards_of).reshape((-1,) + (1,) * (len(extent) - axis_at - 1))

    loudness = one(*split[0])
    for cut in split[1:]:
        loudness = loudness * one(*cut)
    return loudness


def bell_draw(stream_key, dims, spread, most, cuts=(), dtype=jnp.bfloat16):
    gain = shard_levels(stream_key, dims, cuts, -0.22, 0.18) if cuts else 1.0
    drawn = jax.random.normal(stream_key, dims, jnp.float32) * spread * gain
    return jnp.minimum(jnp.maximum(drawn, -most), most).astype(dtype)


def setup_inputs(seed: int = 0, part: int = 0) -> dict:
    arg_keys = jax.random.split(jax.random.key(seed), 15)
    own_keys = jax.random.split(jax.random.fold_in(arg_keys[14], part), 15)
    return {
        "weight_query": bell_draw(own_keys[0], (D_MODEL, Q_DIM), D_MODEL ** -0.5, 0.109375, ((0, 2), (1, 4))),
        "low_query": bell_draw(own_keys[1], (D_MODEL, RANK), D_MODEL ** -0.5, 0.109375, ((0, 2),)),
        "high_query": bell_draw(own_keys[2], (RANK, Q_DIM), RANK ** -0.5, 1.0, ((1, 4),)),
        "weight_key": bell_draw(own_keys[3], (D_MODEL, KV_DIM), D_MODEL ** -0.5, 0.109375, ((0, 2), (1, 4))),
        "low_key": bell_draw(own_keys[4], (D_MODEL, RANK), D_MODEL ** -0.5, 0.109375, ((0, 2),)),
        "high_key": bell_draw(own_keys[5], (RANK, KV_DIM), RANK ** -0.5, 1.0, ((1, 4),)),
        "weight_value": bell_draw(own_keys[6], (D_MODEL, KV_DIM), D_MODEL ** -0.5, 0.109375, ((0, 2), (1, 4))),
        "low_value": bell_draw(own_keys[7], (D_MODEL, RANK), D_MODEL ** -0.5, 0.109375, ((0, 2),)),
        "high_value": bell_draw(own_keys[8], (RANK, KV_DIM), RANK ** -0.5, 1.0, ((1, 4),)),
        "weight_mixed": bell_draw(own_keys[9], (Q_DIM, D_MODEL), Q_DIM ** -0.5, 0.109375, ((0, 4), (1, 2))),
        "low_mixed": bell_draw(own_keys[10], (Q_DIM, RANK), Q_DIM ** -0.5, 0.109375, ((0, 4),)),
        "high_mixed": bell_draw(own_keys[11], (RANK, D_MODEL), RANK ** -0.5, 1.0, ((1, 2),)),
        "norm_train": jnp.clip(1.0 + 0.15 * jax.random.normal(own_keys[12], (D_MODEL,), jnp.float32), 0.25, 1.75),
        "norm_step": jnp.clip(jax.random.uniform(own_keys[13], (D_MODEL,), jnp.float32, -0.3, 0.3) * shard_levels(own_keys[13], (D_MODEL,), ((0, 8),), -0.4, 0.0), -0.3, 0.3),
    }


mix_rate = 2.0


def reference(weight_query, low_query, high_query, weight_key, low_key, high_key, weight_value, low_value, high_value, weight_mixed, low_mixed, high_mixed, norm_train, norm_step):
    whole_query = weight_query.astype(jnp.float32) + mix_rate * jnp.dot(low_query, high_query, preferred_element_type=jnp.float32)
    whole_key = weight_key.astype(jnp.float32) + mix_rate * jnp.dot(low_key, high_key, preferred_element_type=jnp.float32)
    whole_value = weight_value.astype(jnp.float32) + mix_rate * jnp.dot(low_value, high_value, preferred_element_type=jnp.float32)
    whole_mixed = weight_mixed.astype(jnp.float32) + mix_rate * jnp.dot(low_mixed, high_mixed, preferred_element_type=jnp.float32)
    serving_query = whole_query.astype(jnp.bfloat16)
    serving_key = whole_key.astype(jnp.bfloat16)
    serving_value = whole_value.astype(jnp.bfloat16)
    serving_mixed = whole_mixed.astype(jnp.bfloat16)
    serve_norm = (norm_train + norm_step).astype(jnp.bfloat16)
    return serving_query, serving_key, serving_value, serving_mixed, serve_norm
```

```python
import dataclasses
import functools
import math
from typing import Any

import jax
import jax.numpy as jnp
from jax import lax
from jax.experimental import pallas as pl
from jax.experimental.pallas import tpu as pltpu
from jax.sharding import PartitionSpec as P


mix_rate = 2.0
LANES, SUBLANES = 128, 8
CHUNK_BYTES = 800 * 1024
SLACK = 8 << 20

anywhere = pl.BlockSpec(memory_space=pl.ANY)
near = pl.BlockSpec(memory_space=pltpu.VMEM)
written_back = pl.BlockSpec(memory_space=pltpu.VMEM)


def each(count, f):
    def one(j, carry):
        f(j)
        return carry

    lax.fori_loop(0, count, one, 0)


@dataclasses.dataclass
class Item:
    mode: str
    weight: Any
    split: int
    far: bool
    low: Any = None
    high: Any = None
    whole: Any = None
    staged: bool = False

    @property
    def shape(self):
        return self.weight.shape

    @property
    def step(self):
        rows, width = self.shape
        step = min(rows, max(LANES, CHUNK_BYTES // (2 * width) // LANES * LANES))
        while rows % step:
            step -= LANES
        return step

    @property
    def count(self):
        return self.shape[0] // self.step

    def whole_shape(self):
        rows, width = self.shape
        return (2 * rows, width) if self.split == 0 else (rows, 2 * width)


def merge(low, high, weight):
    delta = lax.dot_general(
        low * jnp.bfloat16(mix_rate),
        high,
        (((0,), (0,)), ((), ())),
        preferred_element_type=jnp.float32,
    )
    return (weight.astype(jnp.float32) + delta).astype(jnp.bfloat16)


def run(items, extra):
    arrays, in_specs, outs, out_specs, scratch, aliases = [], [], [], [], [], {}

    def operand(a, spec):
        arrays.append(pltpu.with_memory_space_constraint(a, pltpu.HBM) if spec is anywhere else a)
        in_specs.append(spec)
        return ("in", len(arrays) - 1)

    def result(shape, dtype, spec):
        outs.append(pltpu.VMEM(shape, dtype) if spec is near else jax.ShapeDtypeStruct(shape, dtype))
        out_specs.append(spec)
        return ("out", len(outs) - 1)

    def room(a):
        scratch.append(a)
        return ("scratch", len(scratch) - 1)

    like = lambda a: pltpu.VMEM(a.shape, a.dtype)
    plans = []
    for it in items:
        load = it.mode == "load"
        plan = {"weight": operand(it.weight, anywhere if load else near)}
        if it.mode != "place":
            plan["low"] = operand(it.low, anywhere if load else near)
            plan["high"] = operand(it.high, anywhere if load else near)
            if load:
                plan["held"] = room(like(it.weight))
                plan["held_low"] = room(like(it.low))
                plan["held_high"] = room(like(it.high))
                plan["loaded"] = room(pltpu.SemaphoreType.DMA((it.count + 2,)))
            plan["merged"] = (
                result(it.shape, jnp.bfloat16, near) if it.staged else room(like(it.weight))
            )
        plan["sent"] = room(pltpu.SemaphoreType.DMA((it.count,)))
        plans.append(plan)
    for it, plan in zip(items, plans):
        plan["out"] = result(it.whole_shape(), jnp.bfloat16, anywhere)
        if it.whole is not None:
            aliases[operand(it.whole, anywhere)[1]] = plan["out"][1]
    body, more, shapes, temps = extra or (None, (), (), ())
    more = [operand(a, spec) for a, spec in more]
    made = [result(s.shape, s.dtype, spec) for s, spec in shapes]
    temps = [room(t) for t in temps]

    def kernel(*refs):
        at = {"in": 0, "out": len(arrays), "scratch": len(arrays) + len(outs)}
        ref = lambda place: refs[at[place[0]] + place[1]]
        mine = lax.axis_index("zero")

        def chunk(it, j):
            return pl.ds(pl.multiple_of(j * it.step, it.step), it.step)

        def load(it, plan, j):
            here = chunk(it, j)
            return pltpu.make_async_copy(
                ref(plan["weight"]).at[here, :], ref(plan["held"]).at[here, :], ref(plan["loaded"]).at[j]
            )

        def factors(it, plan):
            return [
                pltpu.make_async_copy(
                    ref(plan[k]), ref(plan["held_" + k]), ref(plan["loaded"]).at[it.count + n]
                )
                for n, k in enumerate(("low", "high"))
            ]

        def store(it, plan, j):
            rows, width = it.shape
            here = chunk(it, j)
            source = 1 - mine if it.far else mine
            if it.split == 0:
                first = pl.multiple_of(source * rows + j * it.step, it.step)
                there = ref(plan["out"]).at[pl.ds(first, it.step), :]
            else:
                there = ref(plan["out"]).at[here, pl.ds(pl.multiple_of(source * width, width), width)]
            merged = ref(plan.get("merged", plan["weight"]))
            return pltpu.make_async_copy(merged.at[here, :], there, ref(plan["sent"]).at[j])

        for it, plan in zip(items, plans):
            if it.mode == "load":
                for copy in factors(it, plan):
                    copy.start()
                each(it.count, lambda j: load(it, plan, j).start())
        for it, plan in zip(items, plans):
            if it.mode == "place":
                each(it.count, lambda j: store(it, plan, j).start())
        for it, plan in zip(items, plans):
            if it.mode == "place":
                continue

            weight, low, high = (plan[k] for k in ("weight", "low", "high"))
            if it.mode == "load":
                weight, low, high = (plan[k] for k in ("held", "held_low", "held_high"))
                for copy in factors(it, plan):
                    copy.wait()

            def work(j):
                if it.mode == "load":
                    load(it, plan, j).wait()
                here = chunk(it, j)
                ref(plan["merged"])[here, :] = merge(
                    ref(low)[:, here], ref(high)[...], ref(weight)[here, :]
                )
                store(it, plan, j).start()

            each(it.count, work)
        if body is not None:
            body(*map(ref, (*more, *made, *temps)))
        for it, plan in zip(items, plans):
            each(it.count, lambda j: store(it, plan, j).wait())

    size = sum(math.prod(it.shape) * 2 for it in items)
    got = pl.pallas_call(
        kernel,
        out_shape=outs,
        in_specs=in_specs,
        out_specs=out_specs,
        scratch_shapes=scratch,
        input_output_aliases=aliases,
        compiler_params=pltpu.CompilerParams(vmem_limit_bytes=2 * size + SLACK),
    )(*arrays)
    wholes = [got[plan["out"][1]] for plan in plans]
    staged = [got[plan["merged"][1]] for it, plan in zip(items, plans) if it.staged]
    return wholes, staged, [got[m[1]] for m in made]


def ring(n, shift):
    return [(i, (i + shift) % n) for i in range(n)]


def met(n, me, s):
    return me ^ s if n & (n - 1) == 0 else (me + n - s) % n


def rounds(n):
    return [[(met(n, i, s), i) for i in range(n)] for s in range(1, n)]


def add_pieces(tile, own_train, own_step, far_train, far_step, out, held, sem):
    rows = own_train.shape[0]
    copies = [
        pltpu.make_async_copy(a, held.at[k], sem.at[k]) for k, a in enumerate((own_train, own_step))
    ]
    for copy in copies:
        copy.start()
    out[...] = jnp.zeros(out.shape, out.dtype)
    for copy in copies:
        copy.wait()
    out[:rows, :] = held[0] + held[1]
    out[tile : tile + rows, :] = far_train[...] + far_step[...]


def lay_out(cols, rows, tile, *refs):
    heard, out, spread = refs[:cols], refs[cols], refs[cols + 1]
    mine, me = lax.axis_index("zero"), lax.axis_index("cols")
    for s in range(cols):
        for half in (0, 1):
            zero = mine if half == 0 else 1 - mine
            column = met(cols, me, s) if cols & (cols - 1) == 0 else lax.rem(me + cols - s, cols)
            at = (zero * cols + column) * rows
            spread[pl.ds(at, rows), :] = heard[s][half * tile : half * tile + rows, :]
    out[...] = spread[...].astype(out.dtype)


def by_pairs(
    sizes,
    weight_query,
    low_query,
    high_query,
    weight_key,
    low_key,
    high_key,
    weight_value,
    low_value,
    high_value,
    weight_mixed,
    low_mixed,
    high_mixed,
    norm_train,
    norm_step,
):
    def swap(a):
        return lax.ppermute(a, "zero", ring(2, 1))

    low_query, low_key, low_value, low_mixed = (
        a.T for a in (low_query, low_key, low_value, low_mixed)
    )
    cols = sizes["cols"]
    rows = norm_train.shape[0] // LANES
    tile = -(-rows // SUBLANES) * SUBLANES
    norms = [a.reshape(rows, LANES) for a in (norm_train, norm_step)]
    far_low_query, far_high_mixed = swap(low_query), swap(high_mixed)
    far_norms = [swap(a) for a in norms]
    far_query, far_mixed = swap(weight_query), swap(weight_mixed)
    wholes, staged, (piece,) = run(
        [
            Item("load", weight_key, 0, False, low_key, high_key, staged=True),
            Item("load", weight_value, 0, False, low_value, high_value, staged=True),
        ],
        (
            functools.partial(add_pieces, tile),
            [(a, anywhere) for a in norms] + [(a, near) for a in far_norms],
            [(jax.ShapeDtypeStruct((2 * tile, LANES), jnp.float32), near)],
            [pltpu.VMEM((2, rows, LANES), jnp.float32), pltpu.SemaphoreType.DMA((2,))],
        ),
    )
    whole_key, whole_value = wholes
    far_key, far_value = (swap(a) for a in staged)
    heard = [piece]
    for pairs in rounds(cols):
        heard.append(lax.ppermute(piece, "cols", pairs))
    (whole_mixed, whole_query), _, _ = run(
        [
            Item("load", weight_mixed, 1, False, low_mixed, high_mixed),
            Item("load", weight_query, 0, False, low_query, high_query),
        ],
        None,
    )
    (mixed, query, key, value), _, (serve_norm,) = run(
        [
            Item("near", far_mixed, 1, True, low_mixed, far_high_mixed, whole_mixed),
            Item("near", far_query, 0, True, far_low_query, high_query, whole_query),
            Item("place", far_key, 0, True, whole=whole_key),
            Item("place", far_value, 0, True, whole=whole_value),
        ],
        (
            functools.partial(lay_out, cols, rows, tile),
            [(a, near) for a in heard],
            [(jax.ShapeDtypeStruct((2 * cols * rows, LANES), jnp.bfloat16), written_back)],
            [pltpu.VMEM((2 * cols * rows, LANES), jnp.float32)],
        ),
    )
    return (query, key, value, mixed, serve_norm.reshape(-1))


def by_gathers(
    weight_query,
    low_query,
    high_query,
    weight_key,
    low_key,
    high_key,
    weight_value,
    low_value,
    high_value,
    weight_mixed,
    low_mixed,
    high_mixed,
    norm_train,
    norm_step,
):
    def served(weight, low, high):
        delta = jnp.dot(low, high, preferred_element_type=jnp.float32)
        return (weight.astype(jnp.float32) + mix_rate * delta).astype(jnp.bfloat16)

    rows = lambda a: lax.all_gather(a, "zero", axis=0, tiled=True)
    columns = lambda a: lax.all_gather(a, "zero", axis=1, tiled=True)
    norm = (norm_train + norm_step).astype(jnp.bfloat16)
    return (
        served(rows(weight_query), rows(low_query), high_query),
        served(rows(weight_key), rows(low_key), high_key),
        served(rows(weight_value), rows(low_value), high_value),
        served(columns(weight_mixed), low_mixed, columns(high_mixed)),
        lax.all_gather(norm, ("zero", "cols"), axis=0, tiled=True),
    )


def on_device(sizes, *args):
    tiled = all(d % LANES == 0 for w in args[0:12:3] for d in w.shape)
    if sizes["zero"] == 2 and tiled and args[12].shape[0] % LANES == 0:
        return by_pairs(sizes, *args)
    return by_gathers(*args)


def solution(mesh):
    placed = (
        P(("job", "zero"), "cols"),
        P(("job", "zero"), None),
        P("job", "cols"),
        P(("job", "zero"), "cols"),
        P(("job", "zero"), None),
        P("job", "cols"),
        P(("job", "zero"), "cols"),
        P(("job", "zero"), None),
        P("job", "cols"),
        P(("job", "cols"), "zero"),
        P(("job", "cols"), None),
        P("job", "zero"),
        P(("job", "zero", "cols")),
        P(("job", "zero", "cols")),
    )
    return jax.shard_map(
        functools.partial(on_device, dict(mesh.shape)),
        mesh=mesh,
        in_specs=placed,
        out_specs=(
            P("job", "cols"),
            P("job", "cols"),
            P("job", "cols"),
            P(("job", "cols"), None),
            P("job"),
        ),
        check_vma=False,
    )
```
